32 devices in a mesh: section: 8 (over z, y), tensor: 4 (over x, core).
Axes of the slice: x: 2, y: 2, z: 4, core: 2. Of those that a mesh axis runs over, the one named last changes fastest.
Arguments:
- inputs: bfloat16 [2, 163840], P(None, 'tensor'), may hold values from -6 to 6
- cotangent: bfloat16 [2, 163840], P(None, 'tensor'), may hold values from -6 to 6
- weights: bfloat16 [8, 2560, 10240], P('section', None, 'tensor'), may hold values from -0.0625 to 0.0625
- norm_gains: float32 [4, 2560], replicated, may hold values from 0.5 to 1.5
Outputs:
- layer_results: bfloat16 [8, 2, 163840], P('section', None, 'tensor')
The draws below stay inside these ranges and needn't reach their ends.
All inputs are finite; a program needn't handle non-finite values.
Results may differ from the reference program's by a relative error of at most 0.02.
Values may be sent and summed in bfloat16 or wider, within the bound.
A program may use at most 64 MiB of HBM per device.

```python
import jax
import jax.numpy as jnp
from jax import lax

D = 2560
FF = 10240
LAYERS = 4
R = 64
M = 2
MB_TOTAL = 2
ALL_LAYERS = 4
N_SECTION = 8
N_TENSOR = 4


def level_of(stream_key, extent, split, least, high):
    gain = 1.0
    for axis_at, blocks in split:
        heights = jax.random.uniform(jax.random.fold_in(jax.random.fold_in(stream_key, 6), axis_at), (blocks,), jnp.float32, least / len(split), high / len(split))
        gain = gain * jnp.repeat(jnp.exp(heights), extent[axis_at] // blocks).reshape((-1,) + (1,) * (len(extent) - 1 - axis_at))
    return gain


def centred(stream_key, shape, width, bound, shards=(), kind=jnp.bfloat16):
    entries = width * jax.random.normal(stream_key, shape, jnp.float32)
    if shards:
        entries = entries * level_of(stream_key, shape, shards, -0.22, 0.18)
    return jnp.clip(entries, -bound, bound).astype(kind)


def setup_inputs(seed: int = 0) -> dict:
    streams_of = jax.random.split(jax.random.key(seed), 5)
    return {
        "inputs": centred(streams_of[0], (MB_TOTAL, R * D), 1.0, 6.0, ((1, 4),)),
        "cotangent": centred(streams_of[1], (MB_TOTAL, R * D), 1.0, 6.0, ((1, 4),)),
        "weights": centred(streams_of[2], (N_SECTION, D, FF), FF ** -0.5, 0.0625, ((0, 8), (2, 4))),
        "norm_gains": jnp.clip(1.0 + 0.1 * jax.random.normal(streams_of[3], (ALL_LAYERS, D), jnp.float32), 0.5, 1.5),
    }


epsilon = 1e-05

def gelu_tanh(values):
    return jax.nn.gelu(values, approximate=True)

def normalize(carried):
    widened = carried.astype(jnp.float32)
    inverse_rms = lax.rsqrt(lax.optimization_barrier(jnp.mean(widened * widened, axis=-1, keepdims=True)) + epsilon)
    return (widened * inverse_rms, inverse_rms)

def block_sum(operand, weight):
    row_total = operand.shape[0]
    feature_count = weight.shape[0]
    block_width = FF // N_TENSOR
    operand_blocks = operand.reshape(row_total, N_TENSOR, block_width).astype(jnp.float32)
    weight_blocks = weight.reshape(feature_count, N_TENSOR, block_width).astype(jnp.float32)
    partials = jnp.einsum('rjb,djb->jrd', operand_blocks, weight_blocks)
    rounded = lax.optimization_barrier(partials.astype(jnp.bfloat16))
    return lax.optimization_barrier(jnp.sum(rounded.astype(jnp.float32), axis=0))

def run_stack(stack_index, stack_count, inputs, cotangent, weights, norm_gains):
    stride = 2 * stack_count
    carried = inputs[stack_index * M:(stack_index + 1) * M].reshape(M * R, D)
    saved_inputs = []
    layer_outputs = []
    for layer_index in range(LAYERS):
        up_weight = weights[layer_index * stride + 2 * stack_index]
        down_weight = weights[layer_index * stride + 2 * stack_index + 1]
        gain_row = norm_gains[stack_index * LAYERS + layer_index]
        unit_rows, _ = normalize(carried)
        normed = (unit_rows * gain_row).astype(jnp.bfloat16)
        preact = jnp.dot(normed, up_weight, preferred_element_type=jnp.float32)
        hidden = gelu_tanh(preact).astype(jnp.bfloat16)
        branch = block_sum(hidden, down_weight)
        saved_inputs.append(carried)
        carried = (carried.astype(jnp.float32) + branch).astype(jnp.bfloat16)
        layer_outputs.append(carried)
    gradient = cotangent[stack_index * M:(stack_index + 1) * M].reshape(M * R, D)
    layer_grads = [None] * LAYERS
    for layer_index in reversed(range(LAYERS)):
        up_weight = weights[layer_index * stride + 2 * stack_index]
        down_weight = weights[layer_index * stride + 2 * stack_index + 1]
        gain_row = norm_gains[stack_index * LAYERS + layer_index]
        grad_hidden = jnp.dot(gradient, down_weight, preferred_element_type=jnp.float32).astype(jnp.bfloat16)
        unit_rows, inverse_rms = normalize(saved_inputs[layer_index])
        normed = (unit_rows * gain_row).astype(jnp.bfloat16)
        preact = jnp.dot(normed, up_weight, preferred_element_type=jnp.float32)
        _, pullback = jax.vjp(gelu_tanh, preact)
        grad_pre = pullback(grad_hidden.astype(jnp.float32))[0].astype(jnp.bfloat16)
        grad_normed = block_sum(grad_pre, up_weight)
        grad_unit = grad_normed * gain_row
        grad_input = inverse_rms * (grad_unit - unit_rows * lax.optimization_barrier(jnp.mean(grad_unit * unit_rows, axis=-1, keepdims=True)))
        gradient = (gradient.astype(jnp.float32) + grad_input).astype(jnp.bfloat16)
        layer_grads[layer_index] = gradient
    return (layer_grads, layer_outputs)

def reference(inputs, cotangent, weights, norm_gains):
    stack_count = N_SECTION // (2 * LAYERS)
    stride = 2 * stack_count
    everything = [None] * N_SECTION
    for stack_index in range(stack_count):
        grads, outputs = run_stack(stack_index, stack_count, inputs, cotangent, weights, norm_gains)
        for layer_index in range(LAYERS):
            position = layer_index * stride + 2 * stack_index
            everything[position] = grads[layer_index].reshape(M, R * D)
            everything[position + 1] = outputs[layer_index].reshape(M, R * D)
    return jnp.stack(everything)
```

```python
import functools

import jax
import jax.numpy as jnp
from jax import lax
from jax.experimental import pallas as pl
from jax.experimental.pallas import tpu as pltpu
from jax.sharding import PartitionSpec as P
LAYERS = 4


epsilon = 1e-05


def swapped(block, axis, stride):
    count = lax.axis_size(axis)
    route = []
    for low in range(count):
        high = low | 1 << stride
        if high != low and high < count:
            route += [(low, high), (high, low)]
    return lax.ppermute(block, axis, route)


def passed_along(block, axis, distance):
    devices = range(lax.axis_size(axis))
    route = [(i - distance, i) for i in devices if i - distance in devices]
    return lax.ppermute(block, axis, route)


def gelu_tanh(values):
    return jax.nn.gelu(values, approximate=True)


def normalize(carried):
    widened = carried.astype(jnp.float32)
    inverse_rms = lax.rsqrt(jnp.mean(widened * widened, axis=-1, keepdims=True) + epsilon)
    return (widened * inverse_rms, inverse_rms)


def project_back(operand, weight):
    return lax.dot_general(
        operand, weight, (((1,), (1,)), ((), ())), preferred_element_type=jnp.float32
    )


def plain_body(inputs, cotangent, weights, norm_gains):
    section_count = lax.axis_size("section")
    tensor_count = lax.axis_size("tensor")
    group_span = 2 * LAYERS
    stack_count = section_count // group_span
    stride = 2 * stack_count
    section_index = lax.axis_index("section")
    tensor_index = lax.axis_index("tensor")
    group_index = section_index % stride // 2
    layer_index = section_index // stride
    up_section = section_index % 2 == 0
    weight_block = weights[0]
    model_width = weight_block.shape[0]
    hidden_width = weight_block.shape[1]
    batch_count = inputs.shape[0] // stack_count
    piece_size = inputs.shape[1]
    row_count = piece_size * tensor_count // model_width
    share_rows = row_count // tensor_count
    own_inputs = lax.dynamic_slice_in_dim(inputs, group_index * batch_count, batch_count, 0)
    own_grads = lax.dynamic_slice_in_dim(cotangent, group_index * batch_count, batch_count, 0)
    full_inputs, full_grads = (
        lax.all_gather(own_inputs, "tensor", axis=1, tiled=True),
        lax.all_gather(own_grads, "tensor", axis=1, tiled=True),
    )
    gain_row = lax.dynamic_index_in_dim(
        norm_gains, group_index * LAYERS + layer_index, 0, keepdims=False
    )
    step_count = batch_count + 2 * LAYERS - 2
    first_layer = layer_index == 0
    last_layer = layer_index == LAYERS - 1

    def in_range(batch):
        return (batch >= 0) & (batch < batch_count)

    def slot_of(batch):
        return jnp.clip(batch, 0, batch_count - 1)

    def put_slot(table, value, slot, valid):
        old_value = lax.dynamic_index_in_dim(table, slot, 0, keepdims=False)
        return lax.dynamic_update_index_in_dim(table, jnp.where(valid, value, old_value), slot, 0)

    def advance(step_index, state_tuple):
        ahead_part, behind_part, stash_rows, parked, results = state_tuple
        ahead_held, behind_held = (
            lax.all_gather(ahead_part, "tensor", axis=0, tiled=True),
            lax.all_gather(behind_part, "tensor", axis=0, tiled=True),
        )
        fwd_batch = step_index - layer_index
        back_batch = step_index - 2 * (LAYERS - 1) + layer_index
        fwd_valid = in_range(fwd_batch)
        back_valid = in_range(back_batch)
        fwd_slot = slot_of(fwd_batch)
        back_slot = slot_of(back_batch)
        entry_block = lax.dynamic_index_in_dim(full_inputs, fwd_slot, 0, keepdims=False).reshape(
            row_count, model_width
        )
        fwd_rows = jnp.where(first_layer, entry_block, ahead_held)
        seed_block = lax.dynamic_index_in_dim(full_grads, back_slot, 0, keepdims=False).reshape(
            row_count, model_width
        )
        back_rows = jnp.where(last_layer, seed_block, behind_held)
        stash_rows = put_slot(stash_rows, fwd_rows, fwd_slot, fwd_valid & up_section)
        saved_rows = lax.dynamic_index_in_dim(stash_rows, back_slot, 0, keepdims=False)
        unit_fwd, _ = normalize(fwd_rows)
        unit_saved, inverse_saved = normalize(saved_rows)
        normed_fwd = (unit_fwd * gain_row).astype(jnp.bfloat16)
        normed_saved = (unit_saved * gain_row).astype(jnp.bfloat16)

        def up_work(operands):
            first_normed, second_normed, grad_rows = operands
            preact_both = jnp.dot(
                jnp.concatenate([first_normed, second_normed], axis=0),
                weight_block,
                preferred_element_type=jnp.float32,
            )
            return (
                gelu_tanh(preact_both[:row_count]).astype(jnp.bfloat16),
                preact_both[row_count:],
            )

        def down_work(operands):
            first_normed, second_normed, grad_rows = operands
            grad_hidden = jnp.dot(
                grad_rows, weight_block, preferred_element_type=jnp.float32
            ).astype(jnp.bfloat16)
            return (grad_hidden, jnp.zeros((row_count, hidden_width), jnp.float32))

        outgoing_hidden, preact_saved = lax.cond(
            up_section, up_work, down_work, (normed_fwd, normed_saved, back_rows)
        )
        incoming_hidden = swapped(outgoing_hidden, "section", 0)
        _, pullback = jax.vjp(gelu_tanh, preact_saved)
        grad_pre = pullback(incoming_hidden.astype(jnp.float32))[0].astype(jnp.bfloat16)
        operand = jnp.where(up_section, grad_pre, incoming_hidden)
        summed = lax.psum_scatter(
            project_back(operand, weight_block)
            .astype(jnp.bfloat16)
            .astype(jnp.float32)
            .astype(jnp.bfloat16),
            "tensor",
            scatter_dimension=0,
            tiled=True,
        ).astype(jnp.float32)
        row_start = tensor_index * share_rows
        fwd_part = lax.dynamic_slice_in_dim(fwd_rows, row_start, share_rows, 0)
        back_part = lax.dynamic_slice_in_dim(back_rows, row_start, share_rows, 0)
        unit_part = lax.dynamic_slice_in_dim(unit_saved, row_start, share_rows, 0)
        inverse_part = lax.dynamic_slice_in_dim(inverse_saved, row_start, share_rows, 0)
        grad_unit = summed * gain_row
        grad_input = inverse_part * (
            grad_unit - unit_part * jnp.mean(grad_unit * unit_part, axis=-1, keepdims=True)
        )
        grad_next = (back_part.astype(jnp.float32) + grad_input).astype(jnp.bfloat16)
        out_next = (fwd_part.astype(jnp.float32) + summed).astype(jnp.bfloat16)
        own_result = jnp.where(up_section, grad_next, out_next)
        partner_part = swapped(own_result, "section", 0)
        done_piece = own_result.reshape(-1)
        out_all = jnp.where(up_section, partner_part, out_next)
        grad_all = jnp.where(up_section, grad_next, partner_part)
        done_slot = jnp.where(up_section, back_slot, fwd_slot)
        done_valid = jnp.where(up_section, back_valid, fwd_valid)
        results = put_slot(results, done_piece, done_slot, done_valid)
        ahead_next = passed_along(out_all, "section", stride)
        behind_next = passed_along(grad_all, "section", -stride)
        return (ahead_next, behind_next, stash_rows, parked, results)

    initial = (
        jnp.zeros((share_rows, model_width), jnp.bfloat16),
        jnp.zeros((share_rows, model_width), jnp.bfloat16),
        jnp.zeros((batch_count, row_count, model_width), jnp.bfloat16),
        jnp.zeros((batch_count, piece_size), jnp.bfloat16),
        jnp.zeros((batch_count, piece_size), jnp.bfloat16),
    )
    finished = lax.fori_loop(0, step_count, advance, initial)
    return finished[4][None]


MESH = pl.DeviceIdType.MESH
ROW_TILE = 16
GELU_C = 0.7978845608028654
GELU_A = 0.044715
PROJECT, COLLECT, FINISH = range(3)


def orders(batches):
    project = [PROJECT * batches + m for m in range(batches)]
    back = []
    for m in range(batches):
        back += [COLLECT * batches + m, FINISH * batches + m]
    turn = []
    for m in range(batches):
        turn += [PROJECT * batches + m]
        if m:
            turn += [FINISH * batches + m - 1]
        turn += [COLLECT * batches + m]
    turn += [FINISH * batches + batches - 1]
    return project + back, turn, back + project, project + back


def relay_kernel(
    sections, tensors, stacks, batches,
    x_ref, g_ref, w_hbm, gain_ref, out_ref,
    w, gathered, resid, normed, hid_out, hid_in, slope, operand, total,
    part_out, part_in, done,
    w_sem, hid_send, hid_recv, part_send, part_recv, row_send, row_recv, res_send, res_recv,
):
    stride = 2 * stacks
    share, width = x_ref.shape[1], x_ref.shape[2]
    chunks, _, piece = w.shape
    rows = tensors * share
    s = lax.axis_index("section")
    t = lax.axis_index("tensor")
    layer = s // stride
    stack = (s % stride) // 2
    is_down = s % 2
    is_up = is_down == 0
    first = layer == 0
    last = layer == LAYERS - 1
    peer = s + 1 - 2 * is_down
    along = s + stride * (2 * is_down - 1)
    behind = s - stride * (2 * is_down - 1)
    target = along + 1 - 2 * is_down
    entry = (is_up & first) | (~is_up & last)
    opening = (is_up & last) | (~is_up & first)
    has_next = ~entry
    has_prev = ~opening

    def weight_copy(c):
        return pltpu.make_async_copy(
            w_hbm.at[:, pl.ds(pl.multiple_of(c * piece, piece), piece)], w.at[c], w_sem.at[c]
        )

    def other(d):
        return lax.rem(t + d, tensors)

    def hid_copy(m, c):
        return pltpu.make_async_remote_copy(
            hid_out.at[m, c], hid_in.at[m, c], hid_send.at[m, c], hid_recv.at[m, c],
            device_id=(peer, t), device_id_type=MESH,
        )

    def part_copy(m, j):
        return pltpu.make_async_remote_copy(
            part_out.at[m, j], part_in.at[m, t], part_send.at[m, j], part_recv.at[m, t],
            device_id=(s, j), device_id_type=MESH,
        )

    def row_copy(m, j, section):
        return pltpu.make_async_remote_copy(
            done.at[m], gathered.at[m, t], row_send.at[m, j], row_recv.at[m, t],
            device_id=(section, j), device_id_type=MESH,
        )

    def res_copy(m):
        return pltpu.make_async_remote_copy(
            done.at[m], resid.at[m], res_send.at[m], res_recv.at[m],
            device_id=(along, t), device_id_type=MESH,
        )

    def start_weight(c, carry):
        weight_copy(c).start()
        return carry

    lax.fori_loop(0, chunks, start_weight, 0)

    barrier = pltpu.get_barrier_semaphore()

    def greet(section, j):
        pl.semaphore_signal(barrier, inc=1, device_id=(section, j), device_id_type=MESH)

    greet(peer, t)
    for d in range(1, tensors):
        greet(s, other(d))

    @pl.when(has_next)
    def _():
        greet(along, t)
        for d in range(tensors):
            greet(target, other(d))

    @pl.when(has_prev)
    def _():
        greet(behind, t)

    next_count = jnp.where(has_next, tensors + 1, 0)
    prev_count = jnp.where(has_prev, 1, 0)
    pl.semaphore_wait(barrier, tensors + next_count + prev_count)

    for m in range(batches):
        at = stack * batches + m

        @pl.when(is_up & first)
        def _():
            done[m] = x_ref[at]

        @pl.when(~is_up & last)
        def _():
            done[m] = g_ref[at]

        @pl.when(is_up & last)
        def _():
            resid[m] = g_ref[at]

        @pl.when(~is_up & first)
        def _():
            resid[m] = x_ref[at]

        @pl.when(entry)
        def _():
            for d in range(1, tensors):
                row_copy(m, other(d), s).start()
            gathered[m, t] = done[m]

    gain = gain_ref[pl.ds(stack * LAYERS + layer, 1), :]
    sequences = orders(batches)

    def project(step, m):
        for d in range(1, tensors):
            j = other(d)
            pltpu.make_async_copy(gathered.at[m, j], gathered.at[m, j], row_recv.at[m, j]).wait()

        @pl.when(has_prev_rows)
        def _():
            pltpu.make_async_copy(gathered.at[m, t], gathered.at[m, t], row_recv.at[m, t]).wait()

        @pl.when(is_up)
        def _():
            for j in range(tensors):
                unit, _ = normalize(gathered[m, j])
                normed[j * share:(j + 1) * share, :] = (unit * gain).astype(jnp.bfloat16)

        @pl.when(~is_up)
        def _():
            for j in range(tensors):
                normed[j * share:(j + 1) * share, :] = gathered[m, j]

        def one(c, carry):
            @pl.when(step == 0)
            def _():
                weight_copy(c).wait()

            value = jnp.dot(normed[...], w[c], preferred_element_type=jnp.float32)

            @pl.when(is_up)
            def _():
                square = value * value
                tanh = jnp.tanh(GELU_C * value * (1.0 + GELU_A * square))
                half = 0.5 * (1.0 + tanh)
                hid_out[m, c] = (value * half).astype(jnp.bfloat16)
                slope[m, c] = half + 0.5 * value * (1.0 - tanh * tanh) * (
                    GELU_C * (1.0 + 3.0 * GELU_A * square)
                )

            @pl.when(~is_up)
            def _():
                hid_out[m, c] = value.astype(jnp.bfloat16)

            hid_copy(m, c).start()
            return carry

        lax.fori_loop(0, chunks, one, 0)

    def collect(step, m):
        total[...] = jnp.zeros_like(total)

        def one(c, carry):
            @pl.when(step == 0)
            def _():
                weight_copy(c).wait()

            hid_copy(m, c).wait_recv()

            @pl.when(is_up)
            def _():
                operand[...] = (hid_in[m, c].astype(jnp.float32) * slope[m, c]).astype(jnp.bfloat16)

            @pl.when(~is_up)
            def _():
                operand[...] = hid_in[m, c]

            for n in range(width // piece):
                cut = slice(n * piece, (n + 1) * piece)
                total[:, cut] += project_back(operand[...], w[c, cut, :])
            return carry

        lax.fori_loop(0, chunks, one, 0)
        for j in range(tensors):
            part_out[m, j] = total[j * share:(j + 1) * share, :].astype(jnp.bfloat16)
        for d in range(1, tensors):
            part_copy(m, other(d)).start()

    def finish(m):
        for d in range(1, tensors):
            j = other(d)
            pltpu.make_async_copy(part_in.at[m, j], part_in.at[m, j], part_recv.at[m, j]).wait()

        summed = part_out[m, t].astype(jnp.float32)
        for d in range(1, tensors):
            summed = summed + part_in[m, other(d)].astype(jnp.float32)

        @pl.when(has_prev)
        def _():
            pltpu.make_async_copy(resid.at[m], resid.at[m], res_recv.at[m]).wait()

        @pl.when(is_up)
        def _():
            unit, inverse = normalize(gathered[m, t])
            grad = summed * gain
            delta = inverse * (grad - unit * jnp.mean(grad * unit, axis=-1, keepdims=True))
            value = (resid[m].astype(jnp.float32) + delta).astype(jnp.bfloat16)
            out_ref[m] = value

        @pl.when(~is_up)
        def _():
            out_ref[m] = (resid[m].astype(jnp.float32) + summed).astype(jnp.bfloat16)

        @pl.when(has_next)
        def _():
            done[m] = out_ref[m]
            for d in range(tensors):
                row_copy(m, other(d), target).start()
            res_copy(m).start()

    has_prev_rows = ~entry

    def advance(step, carry):
        code = 0
        for i in range(3 * batches):
            steady_up, last_up, steady_down, last_down = (table[i] for table in sequences)
            chosen = jnp.where(
                is_up,
                jnp.where(last, last_up, steady_up),
                jnp.where(last, last_down, steady_down),
            )
            code = jnp.where(step == i, chosen, code)
        kind, m = code // batches, code % batches

        @pl.when(kind == PROJECT)
        def _():
            project(step, m)

        @pl.when(kind == COLLECT)
        def _():
            collect(step, m)

        @pl.when(kind == FINISH)
        def _():
            finish(m)

        return carry

    lax.fori_loop(0, 3 * batches, advance, 0)

    def drain(m, carry):
        def drain_hidden(c, inner):
            hid_copy(m, c).wait_send()
            return inner

        lax.fori_loop(0, chunks, drain_hidden, 0)
        for d in range(1, tensors):
            part_copy(m, other(d)).wait_send()

        for d in range(1, tensors):
            row_copy(m, other(d), s).wait_send()

        @pl.when(has_next)
        def _():
            row_copy(m, t, target).wait_send()
            res_copy(m).wait_send()

        return carry

    lax.fori_loop(0, batches, drain, 0)


def relay_body(mesh_shape, inputs, cotangent, weights, norm_gains):
    sections, tensors = mesh_shape["section"], mesh_shape["tensor"]
    stacks = sections // (2 * LAYERS)
    width, hidden = weights.shape[1], weights.shape[2]
    batches = inputs.shape[0] // stacks
    share = inputs.shape[1] // width
    rows = share * tensors
    piece = chunk_of(width, hidden)
    chunks = hidden // piece
    bf16, f32 = jnp.bfloat16, jnp.float32
    dma = pltpu.SemaphoreType.DMA
    vmem = pl.BlockSpec(memory_space=pltpu.VMEM)
    out = pl.pallas_call(
        functools.partial(relay_kernel, sections, tensors, stacks, batches),
        out_shape=jax.ShapeDtypeStruct((batches, share, width), bf16),
        in_specs=[vmem, vmem, pl.BlockSpec(memory_space=pl.ANY), vmem],
        out_specs=vmem,
        scratch_shapes=[
            pltpu.VMEM((chunks, width, piece), bf16),
            pltpu.VMEM((batches, tensors, share, width), bf16),
            pltpu.VMEM((batches, share, width), bf16),
            pltpu.VMEM((rows, width), bf16),
            pltpu.VMEM((batches, chunks, rows, piece), bf16),
            pltpu.VMEM((batches, chunks, rows, piece), bf16),
            pltpu.VMEM((batches, chunks, rows, piece), f32),
            pltpu.VMEM((rows, piece), bf16),
            pltpu.VMEM((rows, width), f32),
            pltpu.VMEM((batches, tensors, share, width), bf16),
            pltpu.VMEM((batches, tensors, share, width), bf16),
            pltpu.VMEM((batches, share, width), bf16),
            dma((chunks,)),
            dma((batches, chunks)),
            dma((batches, chunks)),
            dma((batches, tensors)),
            dma((batches, tensors)),
            dma((batches, tensors)),
            dma((batches, tensors)),
            dma((batches,)),
            dma((batches,)),
        ],
        compiler_params=pltpu.CompilerParams(
            collective_id=0, has_side_effects=True, vmem_limit_bytes=67043328
        ),
    )(
        inputs.reshape(-1, share, width),
        cotangent.reshape(-1, share, width),
        weights[0],
        norm_gains,
    )
    return out.reshape(1, batches, share * width)


def chunk_of(width, hidden):
    for piece in (512, 256, 128):
        if width % piece == 0 and hidden % piece == 0:
            return piece
    return 0


def solution(mesh):
    placed = (P(None, "tensor"), P(None, "tensor"), P("section", None, "tensor"), P())

    def run(inputs, cotangent, weights, norm_gains):
        tensors = mesh.shape["tensor"]
        width, hidden = weights.shape[1], weights.shape[2] // tensors
        local = inputs.shape[1] // tensors
        aligned = local % (ROW_TILE * width) == 0 and chunk_of(width, hidden)
        body = functools.partial(relay_body, dict(mesh.shape)) if aligned else plain_body
        return jax.shard_map(
            body, mesh=mesh, in_specs=placed, out_specs=P("section", None, "tensor"), check_vma=False
        )(inputs, cotangent, weights, norm_gains)

    return run
```

```python
import functools

import jax
import jax.numpy as jnp
from jax import lax
from jax.experimental import pallas as pl
from jax.experimental.pallas import tpu as pltpu
from jax.sharding import PartitionSpec as P
LAYERS = 4


epsilon = 1e-05


def swapped(block, axis, stride):
    count = lax.axis_size(axis)
    route = []
    for low in range(count):
        high = low | 1 << stride
        if high != low and high < count:
            route += [(low, high), (high, low)]
    return lax.ppermute(block, axis, route)


def passed_along(block, axis, distance):
    devices = range(lax.axis_size(axis))
    route = [(i - distance, i) for i in devices if i - distance in devices]
    return lax.ppermute(block, axis, route)


def gelu_tanh(values):
    return jax.nn.gelu(values, approximate=True)


def normalize(carried):
    widened = carried.astype(jnp.float32)
    inverse_rms = lax.rsqrt(jnp.mean(widened * widened, axis=-1, keepdims=True) + epsilon)
    return (widened * inverse_rms, inverse_rms)


def project_back(operand, weight):
    return lax.dot_general(
        operand, weight, (((1,), (1,)), ((), ())), preferred_element_type=jnp.float32
    )


def plain_body(inputs, cotangent, weights, norm_gains):
    section_count = lax.axis_size("section")
    tensor_count = lax.axis_size("tensor")
    group_span = 2 * LAYERS
    stack_count = section_count // group_span
    stride = 2 * stack_count
    section_index = lax.axis_index("section")
    tensor_index = lax.axis_index("tensor")
    group_index = section_index % stride // 2
    layer_index = section_index // stride
    up_section = section_index % 2 == 0
    weight_block = weights[0]
    model_width = weight_block.shape[0]
    hidden_width = weight_block.shape[1]
    batch_count = inputs.shape[0] // stack_count
    piece_size = inputs.shape[1]
    row_count = piece_size * tensor_count // model_width
    share_rows = row_count // tensor_count
    own_inputs = lax.dynamic_slice_in_dim(inputs, group_index * batch_count, batch_count, 0)
    own_grads = lax.dynamic_slice_in_dim(cotangent, group_index * batch_count, batch_count, 0)
    full_inputs, full_grads = (
        lax.all_gather(own_inputs, "tensor", axis=1, tiled=True),
        lax.all_gather(own_grads, "tensor", axis=1, tiled=True),
    )
    gain_row = lax.dynamic_index_in_dim(
        norm_gains, group_index * LAYERS + layer_index, 0, keepdims=False
    )
    step_count = batch_count + 2 * LAYERS - 2
    first_layer = layer_index == 0
    last_layer = layer_index == LAYERS - 1

    def in_range(batch):
        return (batch >= 0) & (batch < batch_count)

    def slot_of(batch):
        return jnp.clip(batch, 0, batch_count - 1)

    def put_slot(table, value, slot, valid):
        old_value = lax.dynamic_index_in_dim(table, slot, 0, keepdims=False)
        return lax.dynamic_update_index_in_dim(table, jnp.where(valid, value, old_value), slot, 0)

    def advance(step_index, state_tuple):
        ahead_part, behind_part, stash_rows, parked, results = state_tuple
        ahead_held, behind_held = (
            lax.all_gather(ahead_part, "tensor", axis=0, tiled=True),
            lax.all_gather(behind_part, "tensor", axis=0, tiled=True),
        )
        fwd_batch = step_index - layer_index
        back_batch = step_index - 2 * (LAYERS - 1) + layer_index
        fwd_valid = in_range(fwd_batch)
        back_valid = in_range(back_batch)
        fwd_slot = slot_of(fwd_batch)
        back_slot = slot_of(back_batch)
        entry_block = lax.dynamic_index_in_dim(full_inputs, fwd_slot, 0, keepdims=False).reshape(
            row_count, model_width
        )
        fwd_rows = jnp.where(first_layer, entry_block, ahead_held)
        seed_block = lax.dynamic_index_in_dim(full_grads, back_slot, 0, keepdims=False).reshape(
            row_count, model_width
        )
        back_rows = jnp.where(last_layer, seed_block, behind_held)
        stash_rows = put_slot(stash_rows, fwd_rows, fwd_slot, fwd_valid & up_section)
        saved_rows = lax.dynamic_index_in_dim(stash_rows, back_slot, 0, keepdims=False)
        unit_fwd, _ = normalize(fwd_rows)
        unit_saved, inverse_saved = normalize(saved_rows)
        normed_fwd = (unit_fwd * gain_row).astype(jnp.bfloat16)
        normed_saved = (unit_saved * gain_row).astype(jnp.bfloat16)

        def up_work(operands):
            first_normed, second_normed, grad_rows = operands
            preact_both = jnp.dot(
                jnp.concatenate([first_normed, second_normed], axis=0),
                weight_block,
                preferred_element_type=jnp.float32,
            )
            return (
                gelu_tanh(preact_both[:row_count]).astype(jnp.bfloat16),
                preact_both[row_count:],
            )

        def down_work(operands):
            first_normed, second_normed, grad_rows = operands
            grad_hidden = jnp.dot(
                grad_rows, weight_block, preferred_element_type=jnp.float32
            ).astype(jnp.bfloat16)
            return (grad_hidden, jnp.zeros((row_count, hidden_width), jnp.float32))

        outgoing_hidden, preact_saved = lax.cond(
            up_section, up_work, down_work, (normed_fwd, normed_saved, back_rows)
        )
        incoming_hidden = swapped(outgoing_hidden, "section", 0)
        _, pullback = jax.vjp(gelu_tanh, preact_saved)
        grad_pre = pullback(incoming_hidden.astype(jnp.float32))[0].astype(jnp.bfloat16)
        operand = jnp.where(up_section, grad_pre, incoming_hidden)
        summed = lax.psum_scatter(
            project_back(operand, weight_block)
            .astype(jnp.bfloat16)
            .astype(jnp.float32)
            .astype(jnp.bfloat16),
            "tensor",
            scatter_dimension=0,
            tiled=True,
        ).astype(jnp.float32)
        row_start = tensor_index * share_rows
        fwd_part = lax.dynamic_slice_in_dim(fwd_rows, row_start, share_rows, 0)
        back_part = lax.dynamic_slice_in_dim(back_rows, row_start, share_rows, 0)
        unit_part = lax.dynamic_slice_in_dim(unit_saved, row_start, share_rows, 0)
        inverse_part = lax.dynamic_slice_in_dim(inverse_saved, row_start, share_rows, 0)
        grad_unit = summed * gain_row
        grad_input = inverse_part * (
            grad_unit - unit_part * jnp.mean(grad_unit * unit_part, axis=-1, keepdims=True)
        )
        grad_next = (back_part.astype(jnp.float32) + grad_input).astype(jnp.bfloat16)
        out_next = (fwd_part.astype(jnp.float32) + summed).astype(jnp.bfloat16)
        own_result = jnp.where(up_section, grad_next, out_next)
        partner_part = swapped(own_result, "section", 0)
        done_piece = own_result.reshape(-1)
        out_all = jnp.where(up_section, partner_part, out_next)
        grad_all = jnp.where(up_section, grad_next, partner_part)
        done_slot = jnp.where(up_section, back_slot, fwd_slot)
        done_valid = jnp.where(up_section, back_valid, fwd_valid)
        results = put_slot(results, done_piece, done_slot, done_valid)
        ahead_next = passed_along(out_all, "section", stride)
        behind_next = passed_along(grad_all, "section", -stride)
        return (ahead_next, behind_next, stash_rows, parked, results)

    initial = (
        jnp.zeros((share_rows, model_width), jnp.bfloat16),
        jnp.zeros((share_rows, model_width), jnp.bfloat16),
        jnp.zeros((batch_count, row_count, model_width), jnp.bfloat16),
        jnp.zeros((batch_count, piece_size), jnp.bfloat16),
        jnp.zeros((batch_count, piece_size), jnp.bfloat16),
    )
    finished = lax.fori_loop(0, step_count, advance, initial)
    return finished[4][None]


MESH = pl.DeviceIdType.MESH
ROW_TILE = 8
GELU_C = 0.7978845608028654
GELU_A = 0.044715
PROJECT, COLLECT, FINISH = range(3)


def orders(batches):
    project = [PROJECT * batches + m for m in range(batches)]
    back, turn = [], []
    for m in range(batches):
        turn += [PROJECT * batches + m]
        for order in (back, turn):
            order += [COLLECT * batches + m]
            if m:
                order += [FINISH * batches + m - 1]
    back += [FINISH * batches + batches - 1]
    turn += [FINISH * batches + batches - 1]
    return project + back, turn, back + project, project + back


def relay_kernel(
    sections, tensors, stacks, batches,
    x_ref, g_ref, w_hbm, gain_ref, out_ref,
    w, gathered, resid, normed, hid_out, hid_in, slope, operand, total,
    part_out, part_in, done,
    w_sem, hid_send, hid_recv, part_send, part_recv, row_send, row_recv, pass_send, res_send, res_recv,
):
    stride = 2 * stacks
    share, width = x_ref.shape[1], x_ref.shape[2]
    chunks, _, piece = w.shape
    rows = tensors * share
    s = lax.axis_index("section")
    t = lax.axis_index("tensor")
    layer = s // stride
    stack = (s % stride) // 2
    is_down = s % 2
    is_up = is_down == 0
    sibling = t + 1 - 2 * (t % 2)
    first = layer == 0
    last = layer == LAYERS - 1
    peer = s + 1 - 2 * is_down
    along = s + stride * (2 * is_down - 1)
    behind = s - stride * (2 * is_down - 1)
    target = along + 1 - 2 * is_down
    entry = (is_up & first) | (~is_up & last)
    opening = (is_up & last) | (~is_up & first)
    has_next = ~entry
    has_prev = ~opening

    def weight_copy(c):
        return pltpu.make_async_copy(
            w_hbm.at[:, pl.ds(pl.multiple_of(c * piece, piece), piece)], w.at[c], w_sem.at[c]
        )

    def other(d):
        return lax.rem(t + d, tensors)

    def hid_copy(m, c):
        return pltpu.make_async_remote_copy(
            hid_out.at[m, c], hid_in.at[m, c], hid_send.at[m, c], hid_recv.at[m, c],
            device_id=(peer, t), device_id_type=MESH,
        )

    def part_copy(m, j):
        return pltpu.make_async_remote_copy(
            part_out.at[m, j], part_in.at[m, t], part_send.at[m, j], part_recv.at[m, t],
            device_id=(s, j), device_id_type=MESH,
        )

    def row_copy(m, j, section):
        return pltpu.make_async_remote_copy(
            done.at[m], gathered.at[m, t], row_send.at[m, j], row_recv.at[m, t],
            device_id=(section, j), device_id_type=MESH,
        )

    def pass_copy(m, i):
        return pltpu.make_async_remote_copy(
            gathered.at[m, i], gathered.at[m, i], pass_send.at[m, i], row_recv.at[m, i],
            device_id=(s, sibling), device_id_type=MESH,
        )

    def row_wait(m, i):
        pltpu.make_async_copy(gathered.at[m, i], gathered.at[m, i], row_recv.at[m, i]).wait()

    def res_copy(m):
        return pltpu.make_async_remote_copy(
            done.at[m], resid.at[m], res_send.at[m], res_recv.at[m],
            device_id=(along, t), device_id_type=MESH,
        )

    def start_weight(c, carry):
        weight_copy(c).start()
        return carry

    lax.fori_loop(0, chunks, start_weight, 0)

    barrier = pltpu.get_barrier_semaphore()

    def greet(section, j):
        pl.semaphore_signal(barrier, inc=1, device_id=(section, j), device_id_type=MESH)

    greet(peer, t)
    for d in range(1, tensors):
        greet(s, other(d))

    @pl.when(has_next)
    def _():
        greet(along, t)
        for d in range(tensors):
            greet(target, other(d))

    @pl.when(has_prev)
    def _():
        greet(behind, t)

    next_count = jnp.where(has_next, tensors + 1, 0)
    prev_count = jnp.where(has_prev, 1, 0)
    pl.semaphore_wait(barrier, tensors + next_count + prev_count)

    for m in range(batches):
        at = stack * batches + m

        @pl.when(is_up & first)
        def _():
            done[m] = x_ref[at]

        @pl.when(~is_up & last)
        def _():
            done[m] = g_ref[at]

        @pl.when(is_up & last)
        def _():
            resid[m] = g_ref[at]

        @pl.when(~is_up & first)
        def _():
            resid[m] = x_ref[at]

        @pl.when(entry)
        def _():
            for d in range(2, tensors, 2):
                row_copy(m, other(d), s).start()
            gathered[m, t] = done[m]

    gain = gain_ref[pl.ds(stack * LAYERS + layer, 1), :]
    sequences = orders(batches)

    def project(step, m):
        @pl.when(has_next)
        def _():
            row_wait(m, t)

        pass_copy(m, t).start()
        for d in range(2, tensors, 2):
            row_wait(m, other(d))
            pass_copy(m, other(d)).start()
        for d in range(0, tensors, 2):
            row_wait(m, lax.rem(sibling + d, tensors))

        @pl.when(is_up)
        def _():
            for j in range(tensors):
                unit, _ = normalize(gathered[m, j])
                normed[j * share:(j + 1) * share, :] = (unit * gain).astype(jnp.bfloat16)

        @pl.when(~is_up)
        def _():
            for j in range(tensors):
                normed[j * share:(j + 1) * share, :] = gathered[m, j]

        def one(c, carry):
            @pl.when(step == 0)
            def _():
                weight_copy(c).wait()

            value = jnp.dot(normed[...], w[c], preferred_element_type=jnp.float32)

            @pl.when(is_up)
            def _():
                square = value * value
                tanh = jnp.tanh(GELU_C * value * (1.0 + GELU_A * square))
                half = 0.5 * (1.0 + tanh)
                hid_out[m, c] = (value * half).astype(jnp.bfloat16)
                slope[m, c] = half + 0.5 * value * (1.0 - tanh * tanh) * (
                    GELU_C * (1.0 + 3.0 * GELU_A * square)
                )

            @pl.when(~is_up)
            def _():
                hid_out[m, c] = value.astype(jnp.bfloat16)

            hid_copy(m, c).start()
            return carry

        lax.fori_loop(0, chunks, one, 0)

    def collect(step, m):
        total[...] = jnp.zeros_like(total)

        def one(c, carry):
            @pl.when(step == 0)
            def _():
                weight_copy(c).wait()

            hid_copy(m, c).wait_recv()

            @pl.when(is_up)
            def _():
                operand[...] = (hid_in[m, c].astype(jnp.float32) * slope[m, c]).astype(jnp.bfloat16)

            @pl.when(~is_up)
            def _():
                operand[...] = hid_in[m, c]

            for n in range(width // piece):
                cut = slice(n * piece, (n + 1) * piece)
                total[:, cut] += project_back(operand[...], w[c, cut, :])
            return carry

        lax.fori_loop(0, chunks, one, 0)
        for j in range(tensors):
            part_out[m, j] = total[j * share:(j + 1) * share, :].astype(jnp.bfloat16)
        for d in range(1, tensors):
            part_copy(m, other(d)).start()

    def finish(m):
        for d in range(1, tensors):
            j = other(d)
            pltpu.make_async_copy(part_in.at[m, j], part_in.at[m, j], part_recv.at[m, j]).wait()

        summed = part_out[m, t].astype(jnp.float32)
        for d in range(1, tensors):
            summed = summed + part_in[m, other(d)].astype(jnp.float32)

        @pl.when(has_prev)
        def _():
            pltpu.make_async_copy(resid.at[m], resid.at[m], res_recv.at[m]).wait()

        @pl.when(is_up)
        def _():
            unit, inverse = normalize(gathered[m, t])
            grad = summed * gain
            delta = inverse * (grad - unit * jnp.mean(grad * unit, axis=-1, keepdims=True))
            value = (resid[m].astype(jnp.float32) + delta).astype(jnp.bfloat16)
            out_ref[m] = value

        @pl.when(~is_up)
        def _():
            out_ref[m] = (resid[m].astype(jnp.float32) + summed).astype(jnp.bfloat16)

        @pl.when(has_next)
        def _():
            done[m] = out_ref[m]
            for d in range(0, tensors, 2):
                row_copy(m, other(d), target).start()
            res_copy(m).start()

    def advance(step, carry):
        code = 0
        for i in range(3 * batches):
            steady_up, last_up, steady_down, last_down = (table[i] for table in sequences)
            chosen = jnp.where(
                is_up,
                jnp.where(last, last_up, steady_up),
                jnp.where(last, last_down, steady_down),
            )
            code = jnp.where(step == i, chosen, code)
        kind, m = code // batches, code % batches

        @pl.when(kind == PROJECT)
        def _():
            project(step, m)

        @pl.when(kind == COLLECT)
        def _():
            collect(step, m)

        @pl.when(kind == FINISH)
        def _():
            finish(m)

        return carry

    lax.fori_loop(0, 3 * batches, advance, 0)

    def drain(m, carry):
        def drain_hidden(c, inner):
            hid_copy(m, c).wait_send()
            return inner

        lax.fori_loop(0, chunks, drain_hidden, 0)
        for d in range(1, tensors):
            part_copy(m, other(d)).wait_send()

        for d in range(2, tensors, 2):
            row_copy(m, other(d), s).wait_send()
        for d in range(0, tensors, 2):
            pass_copy(m, other(d)).wait_send()

        @pl.when(has_next)
        def _():
            row_copy(m, t, target).wait_send()
            res_copy(m).wait_send()

        return carry

    lax.fori_loop(0, batches, drain, 0)


def relay_body(mesh_shape, inputs, cotangent, weights, norm_gains):
    sections, tensors = mesh_shape["section"], mesh_shape["tensor"]
    stacks = sections // (2 * LAYERS)
    width, hidden = weights.shape[1], weights.shape[2]
    split = inputs.shape[1] // (ROW_TILE * width)
    batches = inputs.shape[0] // stacks * split
    share = inputs.shape[1] // (width * split)
    rows = share * tensors
    piece = chunk_of(width, hidden)
    chunks = hidden // piece
    bf16, f32 = jnp.bfloat16, jnp.float32
    dma = pltpu.SemaphoreType.DMA
    vmem = pl.BlockSpec(memory_space=pltpu.VMEM)
    out = pl.pallas_call(
        functools.partial(relay_kernel, sections, tensors, stacks, batches),
        out_shape=jax.ShapeDtypeStruct((batches, share, width), bf16),
        in_specs=[vmem, vmem, pl.BlockSpec(memory_space=pl.ANY), vmem],
        out_specs=vmem,
        scratch_shapes=[
            pltpu.VMEM((chunks, width, piece), bf16),
            pltpu.VMEM((batches, tensors, share, width), bf16),
            pltpu.VMEM((batches, share, width), bf16),
            pltpu.VMEM((rows, width), bf16),
            pltpu.VMEM((batches, chunks, rows, piece), bf16),
            pltpu.VMEM((batches, chunks, rows, piece), bf16),
            pltpu.VMEM((batches, chunks, rows, piece), f32),
            pltpu.VMEM((rows, piece), bf16),
            pltpu.VMEM((rows, width), f32),
            pltpu.VMEM((batches, tensors, share, width), bf16),
            pltpu.VMEM((batches, tensors, share, width), bf16),
            pltpu.VMEM((batches, share, width), bf16),
            dma((chunks,)),
            dma((batches, chunks)),
            dma((batches, chunks)),
            dma((batches, tensors)),
            dma((batches, tensors)),
            dma((batches, tensors)),
            dma((batches, tensors)),
            dma((batches, tensors)),
            dma((batches,)),
            dma((batches,)),
        ],
        compiler_params=pltpu.CompilerParams(
            collective_id=0, has_side_effects=True, vmem_limit_bytes=67043328
        ),
    )(
        inputs.reshape(-1, share, width),
        cotangent.reshape(-1, share, width),
        weights[0],
        norm_gains,
    )
    return out.reshape(1, batches // split, split * share * width)


def chunk_of(width, hidden):
    for piece in (512, 256, 128):
        if width % piece == 0 and hidden % piece == 0:
            return piece
    return 0


def solution(mesh):
    placed = (P(None, "tensor"), P(None, "tensor"), P("section", None, "tensor"), P())

    def run(inputs, cotangent, weights, norm_gains):
        tensors = mesh.shape["tensor"]
        width, hidden = weights.shape[1], weights.shape[2] // tensors
        local = inputs.shape[1] // tensors
        aligned = local % (ROW_TILE * width) == 0 and tensors % 2 == 0 and chunk_of(width, hidden)
        body = functools.partial(relay_body, dict(mesh.shape)) if aligned else plain_body
        return jax.shard_map(
            body, mesh=mesh, in_specs=placed, out_specs=P("section", None, "tensor"), check_vma=False
        )(inputs, cotangent, weights, norm_gains)

    return run
```

```python
import functools

import jax
import jax.numpy as jnp
from jax import lax
from jax.experimental import pallas as pl
from jax.experimental.pallas import tpu as pltpu
from jax.sharding import PartitionSpec as P
LAYERS = 4


epsilon = 1e-05


def swapped(block, axis, stride):
    count = lax.axis_size(axis)
    route = []
    for low in range(count):
        high = low | 1 << stride
        if high != low and high < count:
            route += [(low, high), (high, low)]
    return lax.ppermute(block, axis, route)


def passed_along(block, axis, distance):
    devices = range(lax.axis_size(axis))
    route = [(i - distance, i) for i in devices if i - distance in devices]
    return lax.ppermute(block, axis, route)


def gelu_tanh(values):
    return jax.nn.gelu(values, approximate=True)


def normalize(carried):
    widened = carried.astype(jnp.float32)
    inverse_rms = lax.rsqrt(jnp.mean(widened * widened, axis=-1, keepdims=True) + epsilon)
    return (widened * inverse_rms, inverse_rms)


def project_back(operand, weight):
    return lax.dot_general(
        operand, weight, (((1,), (1,)), ((), ())), preferred_element_type=jnp.float32
    )


def plain_body(inputs, cotangent, weights, norm_gains):
    section_count = lax.axis_size("section")
    tensor_count = lax.axis_size("tensor")
    group_span = 2 * LAYERS
    stack_count = section_count // group_span
    stride = 2 * stack_count
    section_index = lax.axis_index("section")
    tensor_index = lax.axis_index("tensor")
    group_index = section_index % stride // 2
    layer_index = section_index // stride
    up_section = section_index % 2 == 0
    weight_block = weights[0]
    model_width = weight_block.shape[0]
    hidden_width = weight_block.shape[1]
    batch_count = inputs.shape[0] // stack_count
    piece_size = inputs.shape[1]
    row_count = piece_size * tensor_count // model_width
    share_rows = row_count // tensor_count
    own_inputs = lax.dynamic_slice_in_dim(inputs, group_index * batch_count, batch_count, 0)
    own_grads = lax.dynamic_slice_in_dim(cotangent, group_index * batch_count, batch_count, 0)
    full_inputs, full_grads = (
        lax.all_gather(own_inputs, "tensor", axis=1, tiled=True),
        lax.all_gather(own_grads, "tensor", axis=1, tiled=True),
    )
    gain_row = lax.dynamic_index_in_dim(
        norm_gains, group_index * LAYERS + layer_index, 0, keepdims=False
    )
    step_count = batch_count + 2 * LAYERS - 2
    first_layer = layer_index == 0
    last_layer = layer_index == LAYERS - 1

    def in_range(batch):
        return (batch >= 0) & (batch < batch_count)

    def slot_of(batch):
        return jnp.clip(batch, 0, batch_count - 1)

    def put_slot(table, value, slot, valid):
        old_value = lax.dynamic_index_in_dim(table, slot, 0, keepdims=False)
        return lax.dynamic_update_index_in_dim(table, jnp.where(valid, value, old_value), slot, 0)

    def advance(step_index, state_tuple):
        ahead_part, behind_part, stash_rows, parked, results = state_tuple
        ahead_held, behind_held = (
            lax.all_gather(ahead_part, "tensor", axis=0, tiled=True),
            lax.all_gather(behind_part, "tensor", axis=0, tiled=True),
        )
        fwd_batch = step_index - layer_index
        back_batch = step_index - 2 * (LAYERS - 1) + layer_index
        fwd_valid = in_range(fwd_batch)
        back_valid = in_range(back_batch)
        fwd_slot = slot_of(fwd_batch)
        back_slot = slot_of(back_batch)
        entry_block = lax.dynamic_index_in_dim(full_inputs, fwd_slot, 0, keepdims=False).reshape(
            row_count, model_width
        )
        fwd_rows = jnp.where(first_layer, entry_block, ahead_held)
        seed_block = lax.dynamic_index_in_dim(full_grads, back_slot, 0, keepdims=False).reshape(
            row_count, model_width
        )
        back_rows = jnp.where(last_layer, seed_block, behind_held)
        stash_rows = put_slot(stash_rows, fwd_rows, fwd_slot, fwd_valid & up_section)
        saved_rows = lax.dynamic_index_in_dim(stash_rows, back_slot, 0, keepdims=False)
        unit_fwd, _ = normalize(fwd_rows)
        unit_saved, inverse_saved = normalize(saved_rows)
        normed_fwd = (unit_fwd * gain_row).astype(jnp.bfloat16)
        normed_saved = (unit_saved * gain_row).astype(jnp.bfloat16)

        def up_work(operands):
            first_normed, second_normed, grad_rows = operands
            preact_both = jnp.dot(
                jnp.concatenate([first_normed, second_normed], axis=0),
                weight_block,
                preferred_element_type=jnp.float32,
            )
            return (
                gelu_tanh(preact_both[:row_count]).astype(jnp.bfloat16),
                preact_both[row_count:],
            )

        def down_work(operands):
            first_normed, second_normed, grad_rows = operands
            grad_hidden = jnp.dot(
                grad_rows, weight_block, preferred_element_type=jnp.float32
            ).astype(jnp.bfloat16)
            return (grad_hidden, jnp.zeros((row_count, hidden_width), jnp.float32))

        outgoing_hidden, preact_saved = lax.cond(
            up_section, up_work, down_work, (normed_fwd, normed_saved, back_rows)
        )
        incoming_hidden = swapped(outgoing_hidden, "section", 0)
        _, pullback = jax.vjp(gelu_tanh, preact_saved)
        grad_pre = pullback(incoming_hidden.astype(jnp.float32))[0].astype(jnp.bfloat16)
        operand = jnp.where(up_section, grad_pre, incoming_hidden)
        summed = lax.psum_scatter(
            project_back(operand, weight_block)
            .astype(jnp.bfloat16)
            .astype(jnp.float32)
            .astype(jnp.bfloat16),
            "tensor",
            scatter_dimension=0,
            tiled=True,
        ).astype(jnp.float32)
        row_start = tensor_index * share_rows
        fwd_part = lax.dynamic_slice_in_dim(fwd_rows, row_start, share_rows, 0)
        back_part = lax.dynamic_slice_in_dim(back_rows, row_start, share_rows, 0)
        unit_part = lax.dynamic_slice_in_dim(unit_saved, row_start, share_rows, 0)
        inverse_part = lax.dynamic_slice_in_dim(inverse_saved, row_start, share_rows, 0)
        grad_unit = summed * gain_row
        grad_input = inverse_part * (
            grad_unit - unit_part * jnp.mean(grad_unit * unit_part, axis=-1, keepdims=True)
        )
        grad_next = (back_part.astype(jnp.float32) + grad_input).astype(jnp.bfloat16)
        out_next = (fwd_part.astype(jnp.float32) + summed).astype(jnp.bfloat16)
        own_result = jnp.where(up_section, grad_next, out_next)
        partner_part = swapped(own_result, "section", 0)
        done_piece = own_result.reshape(-1)
        out_all = jnp.where(up_section, partner_part, out_next)
        grad_all = jnp.where(up_section, grad_next, partner_part)
        done_slot = jnp.where(up_section, back_slot, fwd_slot)
        done_valid = jnp.where(up_section, back_valid, fwd_valid)
        results = put_slot(results, done_piece, done_slot, done_valid)
        ahead_next = passed_along(out_all, "section", stride)
        behind_next = passed_along(grad_all, "section", -stride)
        return (ahead_next, behind_next, stash_rows, parked, results)

    initial = (
        jnp.zeros((share_rows, model_width), jnp.bfloat16),
        jnp.zeros((share_rows, model_width), jnp.bfloat16),
        jnp.zeros((batch_count, row_count, model_width), jnp.bfloat16),
        jnp.zeros((batch_count, piece_size), jnp.bfloat16),
        jnp.zeros((batch_count, piece_size), jnp.bfloat16),
    )
    finished = lax.fori_loop(0, step_count, advance, initial)
    return finished[4][None]


MESH = pl.DeviceIdType.MESH
ROW_TILE = 8
GELU_C = 0.7978845608028654
GELU_A = 0.044715
PROJECT, COLLECT, FINISH, FLIP = range(4)


def orders(batches):
    project = [PROJECT * batches + m for m in range(batches)]
    back, turn = [], []
    for m in range(batches):
        turn += [PROJECT * batches + m]
        for order in (back, turn):
            order += [COLLECT * batches + m]
            if m:
                order += [FINISH * batches + m - 1]
    back += [FINISH * batches + batches - 1]
    turn += [FINISH * batches + batches - 1]
    flip = [FLIP * batches]
    return project + flip + back, flip + turn, flip + back + project, flip + project + back


def relay_kernel(
    sections, tensors, stacks, batches,
    x_ref, g_ref, w_hbm, gain_ref, out_ref,
    w, flipped, gathered, resid, normed, hid_out, hid_in, slope, operand, total,
    part_out, part_in, done,
    w_sem, hid_send, hid_recv, part_send, part_recv, row_send, row_recv, pass_send, res_send, res_recv,
):
    stride = 2 * stacks
    share, width = x_ref.shape[1], x_ref.shape[2]
    chunks, _, piece = w.shape
    rows = tensors * share
    s = lax.axis_index("section")
    t = lax.axis_index("tensor")
    layer = s // stride
    stack = (s % stride) // 2
    is_down = s % 2
    is_up = is_down == 0
    sibling = t + 1 - 2 * (t % 2)
    first = layer == 0
    last = layer == LAYERS - 1
    peer = s + 1 - 2 * is_down
    along = s + stride * (2 * is_down - 1)
    behind = s - stride * (2 * is_down - 1)
    target = along + 1 - 2 * is_down
    entry = (is_up & first) | (~is_up & last)
    opening = (is_up & last) | (~is_up & first)
    has_next = ~entry
    has_prev = ~opening

    def weight_copy(c):
        return pltpu.make_async_copy(
            w_hbm.at[:, pl.ds(pl.multiple_of(c * piece, piece), piece)], w.at[c], w_sem.at[c]
        )

    def other(d):
        return lax.rem(t + d, tensors)

    def hid_copy(m, c):
        return pltpu.make_async_remote_copy(
            hid_out.at[m, c], hid_in.at[m, c], hid_send.at[m, c], hid_recv.at[m, c],
            device_id=(peer, t), device_id_type=MESH,
        )

    def part_copy(m, j):
        return pltpu.make_async_remote_copy(
            part_out.at[m, j], part_in.at[m, t], part_send.at[m, j], part_recv.at[m, t],
            device_id=(s, j), device_id_type=MESH,
        )

    def row_copy(m, j, section):
        return pltpu.make_async_remote_copy(
            done.at[m], gathered.at[m, t], row_send.at[m, j], row_recv.at[m, t],
            device_id=(section, j), device_id_type=MESH,
        )

    def pass_copy(m, i):
        return pltpu.make_async_remote_copy(
            gathered.at[m, i], gathered.at[m, i], pass_send.at[m, i], row_recv.at[m, i],
            device_id=(s, sibling), device_id_type=MESH,
        )

    def row_wait(m, i):
        pltpu.make_async_copy(gathered.at[m, i], gathered.at[m, i], row_recv.at[m, i]).wait()

    def res_copy(m):
        return pltpu.make_async_remote_copy(
            done.at[m], resid.at[m], res_send.at[m], res_recv.at[m],
            device_id=(along, t), device_id_type=MESH,
        )

    def start_weight(c, carry):
        weight_copy(c).start()
        return carry

    lax.fori_loop(0, chunks, start_weight, 0)

    barrier = pltpu.get_barrier_semaphore()

    def greet(section, j):
        pl.semaphore_signal(barrier, inc=1, device_id=(section, j), device_id_type=MESH)

    greet(peer, t)
    for d in range(1, tensors):
        greet(s, other(d))

    @pl.when(has_next)
    def _():
        greet(along, t)
        for d in range(tensors):
            greet(target, other(d))

    @pl.when(has_prev)
    def _():
        greet(behind, t)

    next_count = jnp.where(has_next, tensors + 1, 0)
    prev_count = jnp.where(has_prev, 1, 0)
    pl.semaphore_wait(barrier, tensors + next_count + prev_count)

    for m in range(batches):
        at = stack * batches + m

        @pl.when(is_up & first)
        def _():
            done[m] = x_ref[at]

        @pl.when(~is_up & last)
        def _():
            done[m] = g_ref[at]

        @pl.when(is_up & last)
        def _():
            resid[m] = g_ref[at]

        @pl.when(~is_up & first)
        def _():
            resid[m] = x_ref[at]

        @pl.when(entry)
        def _():
            for d in range(2, tensors, 2):
                row_copy(m, other(d), s).start()
            gathered[m, t] = done[m]

    gain = gain_ref[pl.ds(stack * LAYERS + layer, 1), :]
    sequences = orders(batches)

    def project(step, m):
        @pl.when(has_next)
        def _():
            row_wait(m, t)

        pass_copy(m, t).start()
        for d in range(2, tensors, 2):
            row_wait(m, other(d))
            pass_copy(m, other(d)).start()
        for d in range(0, tensors, 2):
            row_wait(m, lax.rem(sibling + d, tensors))

        @pl.when(is_up)
        def _():
            for j in range(tensors):
                unit, _ = normalize(gathered[m, j])
                normed[j * share:(j + 1) * share, :] = (unit * gain).astype(jnp.bfloat16)

        @pl.when(~is_up)
        def _():
            for j in range(tensors):
                normed[j * share:(j + 1) * share, :] = gathered[m, j]

        def one(c, carry):
            @pl.when(step == 0)
            def _():
                weight_copy(c).wait()

            value = jnp.dot(normed[...], w[c], preferred_element_type=jnp.float32)

            @pl.when(is_up)
            def _():
                square = value * value
                tanh = jnp.tanh(GELU_C * value * (1.0 + GELU_A * square))
                half = 0.5 * (1.0 + tanh)
                hid_out[m, c] = (value * half).astype(jnp.bfloat16)
                slope[m, c] = half + 0.5 * value * (1.0 - tanh * tanh) * (
                    GELU_C * (1.0 + 3.0 * GELU_A * square)
                )

            @pl.when(~is_up)
            def _():
                hid_out[m, c] = value.astype(jnp.bfloat16)

            hid_copy(m, c).start()
            return carry

        lax.fori_loop(0, chunks, one, 0)

    def flip(step):
        def one(c, carry):
            @pl.when(step == 0)
            def _():
                weight_copy(c).wait()

            def block(n, inner):
                at = pl.ds(pl.multiple_of(n * piece, piece), piece)
                flipped[c, :, at] = w[c, at, :].T
                return inner

            return lax.fori_loop(0, width // piece, block, carry)

        lax.fori_loop(0, chunks, one, 0)

    def collect(m):
        total[...] = jnp.zeros_like(total)

        def one(c, carry):
            hid_copy(m, c).wait_recv()

            @pl.when(is_up)
            def _():
                operand[...] = (hid_in[m, c].astype(jnp.float32) * slope[m, c]).astype(jnp.bfloat16)

            @pl.when(~is_up)
            def _():
                operand[...] = hid_in[m, c]

            for n in range(width // piece):
                cut = slice(n * piece, (n + 1) * piece)
                total[:, cut] += jnp.dot(
                    operand[...], flipped[c, :, cut], preferred_element_type=jnp.float32
                )
            return carry

        lax.fori_loop(0, chunks, one, 0)
        for j in range(tensors):
            part_out[m, j] = total[j * share:(j + 1) * share, :].astype(jnp.bfloat16)
        for d in range(1, tensors):
            part_copy(m, other(d)).start()

    def finish(m):
        for d in range(1, tensors):
            j = other(d)
            pltpu.make_async_copy(part_in.at[m, j], part_in.at[m, j], part_recv.at[m, j]).wait()

        summed = part_out[m, t].astype(jnp.float32)
        for d in range(1, tensors):
            summed = summed + part_in[m, other(d)].astype(jnp.float32)

        @pl.when(has_prev)
        def _():
            pltpu.make_async_copy(resid.at[m], resid.at[m], res_recv.at[m]).wait()

        @pl.when(is_up)
        def _():
            unit, inverse = normalize(gathered[m, t])
            grad = summed * gain
            delta = inverse * (grad - unit * jnp.mean(grad * unit, axis=-1, keepdims=True))
            value = (resid[m].astype(jnp.float32) + delta).astype(jnp.bfloat16)
            out_ref[m] = value

        @pl.when(~is_up)
        def _():
            out_ref[m] = (resid[m].astype(jnp.float32) + summed).astype(jnp.bfloat16)

        @pl.when(has_next)
        def _():
            done[m] = out_ref[m]
            for d in range(0, tensors, 2):
                row_copy(m, other(d), target).start()
            res_copy(m).start()

    def advance(step, carry):
        code = 0
        for i in range(len(sequences[0])):
            steady_up, last_up, steady_down, last_down = (table[i] for table in sequences)
            chosen = jnp.where(
                is_up,
                jnp.where(last, last_up, steady_up),
                jnp.where(last, last_down, steady_down),
            )
            code = jnp.where(step == i, chosen, code)
        kind, m = code // batches, code % batches

        @pl.when(kind == PROJECT)
        def _():
            project(step, m)

        @pl.when(kind == COLLECT)
        def _():
            collect(m)

        @pl.when(kind == FLIP)
        def _():
            flip(step)

        @pl.when(kind == FINISH)
        def _():
            finish(m)

        return carry

    lax.fori_loop(0, len(sequences[0]), advance, 0)

    def drain(m, carry):
        def drain_hidden(c, inner):
            hid_copy(m, c).wait_send()
            return inner

        lax.fori_loop(0, chunks, drain_hidden, 0)
        for d in range(1, tensors):
            part_copy(m, other(d)).wait_send()

        for d in range(2, tensors, 2):
            row_copy(m, other(d), s).wait_send()
        for d in range(0, tensors, 2):
            pass_copy(m, other(d)).wait_send()

        @pl.when(has_next)
        def _():
            row_copy(m, t, target).wait_send()
            res_copy(m).wait_send()

        return carry

    lax.fori_loop(0, batches, drain, 0)


def relay_body(mesh_shape, inputs, cotangent, weights, norm_gains):
    sections, tensors = mesh_shape["section"], mesh_shape["tensor"]
    stacks = sections // (2 * LAYERS)
    width, hidden = weights.shape[1], weights.shape[2]
    split = inputs.shape[1] // (ROW_TILE * width)
    batches = inputs.shape[0] // stacks * split
    share = inputs.shape[1] // (width * split)
    rows = share * tensors
    piece = chunk_of(width, hidden)
    chunks = hidden // piece
    bf16, f32 = jnp.bfloat16, jnp.float32
    dma = pltpu.SemaphoreType.DMA
    vmem = pl.BlockSpec(memory_space=pltpu.VMEM)
    out = pl.pallas_call(
        functools.partial(relay_kernel, sections, tensors, stacks, batches),
        out_shape=jax.ShapeDtypeStruct((batches, share, width), bf16),
        in_specs=[vmem, vmem, pl.BlockSpec(memory_space=pl.ANY), vmem],
        out_specs=vmem,
        scratch_shapes=[
            pltpu.VMEM((chunks, width, piece), bf16),
            pltpu.VMEM((chunks, piece, width), bf16),
            pltpu.VMEM((batches, tensors, share, width), bf16),
            pltpu.VMEM((batches, share, width), bf16),
            pltpu.VMEM((rows, width), bf16),
            pltpu.VMEM((batches, chunks, rows, piece), bf16),
            pltpu.VMEM((batches, chunks, rows, piece), bf16),
            pltpu.VMEM((batches, chunks, rows, piece), f32),
            pltpu.VMEM((rows, piece), bf16),
            pltpu.VMEM((rows, width), f32),
            pltpu.VMEM((batches, tensors, share, width), bf16),
            pltpu.VMEM((batches, tensors, share, width), bf16),
            pltpu.VMEM((batches, share, width), bf16),
            dma((chunks,)),
            dma((batches, chunks)),
            dma((batches, chunks)),
            dma((batches, tensors)),
            dma((batches, tensors)),
            dma((batches, tensors)),
            dma((batches, tensors)),
            dma((batches, tensors)),
            dma((batches,)),
            dma((batches,)),
        ],
        compiler_params=pltpu.CompilerParams(
            collective_id=0, has_side_effects=True, vmem_limit_bytes=67043328
        ),
    )(
        inputs.reshape(-1, share, width),
        cotangent.reshape(-1, share, width),
        weights[0],
        norm_gains,
    )
    return out.reshape(1, batches // split, split * share * width)


def chunk_of(width, hidden):
    for piece in (512, 256, 128):
        if width % piece == 0 and hidden % piece == 0:
            return piece
    return 0


def solution(mesh):
    placed = (P(None, "tensor"), P(None, "tensor"), P("section", None, "tensor"), P())

    def run(inputs, cotangent, weights, norm_gains):
        tensors = mesh.shape["tensor"]
        width, hidden = weights.shape[1], weights.shape[2] // tensors
        local = inputs.shape[1] // tensors
        aligned = local % (ROW_TILE * width) == 0 and tensors % 2 == 0 and chunk_of(width, hidden)
        body = functools.partial(relay_body, dict(mesh.shape)) if aligned else plain_body
        return jax.shard_map(
            body, mesh=mesh, in_specs=placed, out_specs=P("section", None, "tensor"), check_vma=False
        )(inputs, cotangent, weights, norm_gains)

    return run
```
